128 devices in a mesh: grp: 8 (over y, core), mem: 16 (over x, z).
Axes of the slice: x: 4, y: 4, z: 4, core: 2. Of those that a mesh axis runs over, the one named last changes fastest.
Arguments:
- factors: bfloat16 [256, 288, 1792], P(('grp', 'mem')), may hold values from -3 to 3
- screen: int32 [128, 18], P(('grp', 'mem')), may hold values from 0 to 1, as said below
Outputs:
- exchange_matrix: float32 [1792, 1792], P(('grp', 'mem'))
The draws below stay inside these ranges and needn't reach their ends.
Inputs may be any that keep to these rules, and one draw needn't show every extreme that they name: screen[b, j] is 1 where auxiliary block b and occupied block j survive screening; every auxiliary block keeps at least one occupied block.
All inputs are finite; a program needn't handle non-finite values.
Results may differ from the reference program's by a relative error of at most 0.0003.
Values may be sent and summed in bfloat16 or wider, within the bound.
A program may use at most 128 MiB of HBM per device.

```python
import jax
import jax.numpy as jnp
from jax import lax

NBF = 1792
NOCC = 288
NOB = 18
NAB = 128
NAUX = 256


def draw_screen(key, part):
    count_key = jax.random.fold_in(key, 11)
    shuffle_key = jax.random.fold_in(key, 23)
    kept_count = jax.random.randint(count_key, (NAB, 1), 1, NOB + 1)
    row_keys = jax.random.split(shuffle_key, NAB)

    def shuffle_row(row_key):
        return jax.random.permutation(row_key, NOB)
    shuffled = jax.vmap(shuffle_row)(row_keys)
    position = jnp.argsort(shuffled, axis=1)
    return (position < kept_count).astype(jnp.int32)


def with_spikes(array, own_key, source, target, blocks, factor):
    def block_of(dim):
        return (jnp.arange(array.shape[dim]) // (array.shape[dim] // blocks)).reshape((-1,) + (1,) * (array.ndim - 1 - dim))

    near = jax.random.permutation(own_key, blocks)[block_of(target)]
    second = (block_of(target) + blocks // 2) % blocks
    return jnp.where((block_of(source) == near) | (block_of(source) == second), factor * array, array)


def steps_of(own_key, extent, pieces, low, top_value):
    def one(axis_at, parts):
        draws = jax.random.uniform(jax.random.fold_in(jax.random.fold_in(own_key, 6), axis_at), (parts,), jnp.float32, low / len(pieces), top_value / len(pieces))
        return jnp.repeat(jnp.exp(draws), extent[axis_at] // parts).reshape((-1,) + (1,) * (len(extent) - axis_at - 1))

    level = one(*pieces[0])
    for cut in pieces[1:]:
        level = level * one(*cut)
    return level


def bell_draw_with(own_key, dims, width, most, cuts, heavy, dtype=jnp.bfloat16):
    values = width * jax.random.normal(own_key, dims, jnp.float32)
    if cuts:
        values = values * steps_of(own_key, dims, cuts, -0.22, 0.18)
    return jnp.clip(with_spikes(values, jax.random.fold_in(own_key, 3), *heavy), -most, most).astype(dtype)


def setup_inputs(seed: int = 0) -> dict:
    keys = jax.random.split(jax.random.key(seed), 3)
    factors = bell_draw_with(keys[0], (NAUX, NOCC, NBF), 0.05, 3.0, ((0, 128),), (0, 2, 128, 5.5))
    screen = draw_screen(jax.random.fold_in(keys[2], 71), 0)
    return {"factors": factors, "screen": screen}


def reference(factors, screen):
    total_aux, occ_count, basis = factors.shape
    block_count, occ_blocks = screen.shape
    aux_rows = total_aux // block_count
    occ_width = occ_count // occ_blocks
    grouped = factors.reshape(block_count, aux_rows, occ_blocks, occ_width, basis)

    def add_block(running, pair):
        block, flags = pair
        masked = block * flags.astype(jnp.bfloat16)[None, :, None, None]
        flat_rows = masked.reshape(-1, basis)
        return running + jnp.dot(flat_rows.T, flat_rows, preferred_element_type=jnp.float32), None

    result, _ = lax.scan(add_block, jnp.zeros((basis, basis), jnp.float32), (grouped, screen))
    return result
```

```python
import jax
import jax.numpy as jnp
from jax import lax
from jax.experimental import pallas as pl
from jax.experimental.pallas import tpu as pltpu
from jax.sharding import PartitionSpec as P

MESH = pl.DeviceIdType.MESH
NBF = 1792
ROWS = 576
DEPTH = 640
TOP = 32000.0
X, Y, Z = 0, 1, 2
COLOURS = (
    ((X, Y, Z), 0, 640, 56, 14),
    ((Y, Z, X), 640, 640, 56, 14),
    ((Z, X, Y), 1280, 512, 64, 16),
)
HOPS = (1, 3, 2)


def encoded(value, inverse):
    level = lax.rsqrt(lax.rsqrt(jnp.abs(value) * inverse)) * TOP + 0.5
    code = level.astype(jnp.int32)
    return jnp.where(value < 0.0, -code, code).astype(jnp.int16)


def decoded(code, scale):
    level = code.astype(jnp.int32).astype(jnp.float32)
    return level * jnp.abs(level) * (level * level) * scale


def kernel(
    f_ref, s_ref, o_ref,
    fbuf, pick, t1, ft0, ft1, ft2, whole,
    q10, q11, q12, r10, r11, r12, a0, a1, a2,
    q20, q21, q22, r20, r21, r22,
    b0, b1, b2, q30, q31, q32, r30, r31, r32,
    peer_screen, sc_own, sc_peer, sc1, sc2s, sc2, sc3s, sc3,
    load_sem, swap_send, swap_recv, send1, recv1, send2, recv2, send3, recv3,
    ssend1, srecv1, ssend2, srecv2, ssend3, srecv3,
):
    grp, mem = lax.axis_index("grp"), lax.axis_index("mem")
    here = (mem // 4, grp // 2, mem % 4)
    core = grp % 2

    def along(axis, hop):
        at = list(here)
        at[axis] = (at[axis] + hop) % 4
        return (at[Y] * 2 + core, at[X] * 4 + at[Z])

    peer = (here[Y] * 2 + 1 - core, mem)

    loads = [
        pltpu.make_async_copy(f_ref.at[i], fbuf.at[pl.ds(i * 288, 288)], load_sem.at[i])
        for i in range(2)
    ]
    for load in loads:
        load.start()

    barrier = pltpu.get_barrier_semaphore()
    pl.semaphore_signal(barrier, inc=1, device_id=peer, device_id_type=MESH)
    for axis in range(3):
        for hop in HOPS:
            pl.semaphore_signal(barrier, inc=1, device_id=along(axis, hop), device_id_type=MESH)

    def where_from(rows, first, kind):
        r = lax.broadcasted_iota(jnp.int32, (rows, 384), 0).astype(jnp.float32)
        l = lax.broadcasted_iota(jnp.int32, (rows, 384), 1).astype(jnp.float32)
        if kind == 0:
            n = r
        else:
            w = 14.0 if kind == 1 else 16.0
            z = jnp.floor((r + 0.5) * (1.0 / (4 * w)))
            x = jnp.floor((r - z * (4 * w) + 0.5) * (1.0 / w))
            i = r - z * (4 * w) - x * w
            n = jnp.where(i < 14.0, x * 56.0 + z * 14.0 + i, 4096.0)
        pick[pl.ds(first, rows), :] = l - n

    where_from(224, 0, 0)
    where_from(224, 224, 1)
    where_from(256, 448, 2)
    zero_rows = jnp.zeros((DEPTH - ROWS, NBF), jnp.bfloat16)
    fbuf[pl.ds(ROWS, DEPTH - ROWS), :] = zero_rows
    fbuf[pl.ds(DEPTH + ROWS, DEPTH - ROWS), :] = zero_rows

    pl.semaphore_wait(barrier, 10)
    swaps = [
        pltpu.make_async_remote_copy(
            src_ref=f_ref.at[i], dst_ref=fbuf.at[pl.ds(DEPTH + i * 288, 288)],
            send_sem=swap_send.at[i], recv_sem=swap_recv.at[i], device_id=peer, device_id_type=MESH,
        )
        for i in range(2)
    ]
    swaps.append(
        pltpu.make_async_remote_copy(
            src_ref=s_ref, dst_ref=peer_screen, send_sem=swap_send.at[2], recv_sem=swap_recv.at[2],
            device_id=peer, device_id_type=MESH,
        )
    )
    for swap in swaps:
        swap.start()

    k = lax.broadcasted_iota(jnp.int32, (18, DEPTH), 1)
    j = lax.broadcasted_iota(jnp.int32, (18, DEPTH), 0) * 16
    k = jnp.where(k >= 288, k - 288, k)
    spread = jnp.where((k >= j) & (k < j + 16), 1.0, 0.0).astype(jnp.bfloat16)

    def mask_of(ref):
        kept = jnp.where(ref[...] == 1, 1.0, 0.0).astype(jnp.bfloat16)
        kept = jnp.broadcast_to(kept, (16, 18))
        m = jnp.dot(kept, spread, preferred_element_type=jnp.float32)
        lane = lax.broadcasted_iota(jnp.int32, (16, DEPTH), 1)
        return jnp.where(lane < ROWS, m, 0.0)

    def prepare(first, mask):
        def one(y, _):
            g = 2 * y + core
            tile = (224 * g) // 128 - g // 7
            off = 224 * g - 128 * tile
            window = fbuf[pl.ds(first, DEPTH), pl.ds(pl.multiple_of(tile * 128, 128), 384)]
            offset = off.astype(jnp.float32)

            def taken(at, rows):
                chosen = jnp.where(pick[pl.ds(at, rows), :] == offset, 1.0, 0.0).astype(jnp.bfloat16)
                got = lax.dot_general(
                    chosen, window, (((1,), (1,)), ((), ())), preferred_element_type=jnp.float32
                )
                return got * mask[0:1]

            columns = pl.ds(first, DEPTH)
            ft0[y, :, columns] = taken(0, 224).astype(jnp.bfloat16)
            got = taken(224, 224)
            for z in range(4):
                t1[z, y] = got[z * 56 : z * 56 + 56]
            got = taken(448, 256).astype(jnp.bfloat16)
            for z in range(4):
                for x in range(4):
                    at = (z * 4 + x) * 16
                    ft2[x, z, y, :, columns] = got[at : at + 16]
            return 0

        lax.fori_loop(0, 4, one, 0)
        for z in range(4):
            ft1[z, :, pl.ds(first, DEPTH)] = t1[z].reshape(224, DEPTH).astype(jnp.bfloat16)

    for load in loads:
        load.wait()
    own_mask = mask_of(s_ref)
    own = fbuf[pl.ds(0, DEPTH), :]
    squares = jnp.dot(own_mask.astype(jnp.bfloat16), own * own, preferred_element_type=jnp.float32)
    most = jnp.max(squares[0:8], axis=1, keepdims=True) * 1.02 + 1e-30
    sc_own[...] = jnp.broadcast_to(most, (8, 128))
    scale_swap = pltpu.make_async_remote_copy(
        src_ref=sc_own, dst_ref=sc_peer, send_sem=swap_send.at[3], recv_sem=swap_recv.at[3],
        device_id=peer, device_id_type=MESH,
    )
    scale_swap.start()
    swaps.append(scale_swap)
    prepare(0, own_mask)
    scale_swap.wait_recv()
    mine = sc_own[...] + sc_peer[...]

    sent = []
    sc1[9] = mine
    for axis in range(3):
        for hop in HOPS:
            copy = pltpu.make_async_remote_copy(
                src_ref=sc1.at[9], dst_ref=sc1.at[axis * 3 + hop - 1],
                send_sem=ssend1.at[axis * 3 + hop - 1], recv_sem=srecv1.at[axis * 3 + hop - 1],
                device_id=along(axis, hop), device_id_type=MESH,
            )
            copy.start()
            sent.append(copy)
    scale_copies1 = list(sent)

    for swap in swaps[:3]:
        swap.wait_recv()
    prepare(DEPTH, mask_of(peer_screen))

    q1, r1, a = (q10, q11, q12), (r10, r11, r12), (a0, a1, a2)
    q2, r2, b = (q20, q21, q22), (r20, r21, r22), (b0, b1, b2)
    q3, r3 = (q30, q31, q32), (r30, r31, r32)
    inverse = (1.0 / mine)[0:1, 0:1]

    first_copies = {}
    for step, hop2 in enumerate((1, 3, 2, 0)):
        for c, (axes, col, cols, rows, _) in enumerate(COLOURS):
            v = (here[axes[1]] + hop2) % 4
            lhs = ft0[v] if c == 0 else ft1[v] if c == 1 else ft2[v].reshape(256, 2 * DEPTH)
            made = jnp.dot(lhs, fbuf[:, pl.ds(col, cols)], preferred_element_type=jnp.float32)
            whole[:, pl.ds(0, rows), pl.ds(0, cols)] = made.reshape(4, rows, cols)
            for hop in HOPS:
                u = (here[axes[0]] + hop) % 4
                q1[c][hop - 1, step] = encoded(whole[u, pl.ds(0, rows), pl.ds(0, cols)], inverse)
                copy = pltpu.make_async_remote_copy(
                    src_ref=q1[c].at[hop - 1, step], dst_ref=r1[c].at[hop - 1, step],
                    send_sem=send1.at[c, hop - 1, step], recv_sem=recv1.at[c, hop - 1, step],
                    device_id=along(axes[0], hop), device_id_type=MESH,
                )
                copy.start()
                sent.append(copy)
                first_copies[c, hop, step] = copy
            a[c][step] = whole[here[axes[0]], pl.ds(0, rows), pl.ds(0, cols)]

    for copy in scale_copies1:
        copy.wait_recv()
    unit = 1.0 / (TOP * TOP) / (TOP * TOP)
    scale2_copies = []
    for c, (axes, *_) in enumerate(COLOURS):
        at = axes[0] * 3
        sc2s[c] = mine + sc1[at] + sc1[at + 1] + sc1[at + 2]
        for hop in HOPS:
            copy = pltpu.make_async_remote_copy(
                src_ref=sc2s.at[c], dst_ref=sc2.at[c, hop - 1],
                send_sem=ssend2.at[c, hop - 1], recv_sem=srecv2.at[c, hop - 1],
                device_id=along(axes[1], hop), device_id_type=MESH,
            )
            copy.start()
            sent.append(copy)
            scale2_copies.append(copy)

    second_copies = {}

    def summed1(c, step):
        axes = COLOURS[c][0]
        total = a[c][step]
        for hop in HOPS:
            first_copies[c, hop, step].wait_recv()
            scale = sc1[axes[0] * 3 + hop - 1][0:1, 0:1] * unit
            total = total + decoded(r1[c][hop - 1, step], scale)
        return total

    for step, hop2 in enumerate(HOPS):
        for c, (axes, *_) in enumerate(COLOURS):
            inv2 = (1.0 / sc2s[c])[0:1, 0:1]
            q2[c][hop2 - 1] = encoded(summed1(c, step), inv2)
            copy = pltpu.make_async_remote_copy(
                src_ref=q2[c].at[hop2 - 1], dst_ref=r2[c].at[hop2 - 1],
                send_sem=send2.at[c, hop2 - 1], recv_sem=recv2.at[c, hop2 - 1],
                device_id=along(axes[1], hop2), device_id_type=MESH,
            )
            copy.start()
            sent.append(copy)
            second_copies[c, hop2] = copy

    for copy in scale2_copies:
        copy.wait_recv()
    scale3_copies = []
    for c, (axes, *_) in enumerate(COLOURS):
        sc3s[c] = sc2s[c] + sc2[c, 0] + sc2[c, 1] + sc2[c, 2]
        for hop in HOPS:
            copy = pltpu.make_async_remote_copy(
                src_ref=sc3s.at[c], dst_ref=sc3.at[c, hop - 1],
                send_sem=ssend3.at[c, hop - 1], recv_sem=srecv3.at[c, hop - 1],
                device_id=along(axes[2], hop), device_id_type=MESH,
            )
            copy.start()
            sent.append(copy)
            scale3_copies.append(copy)

    for c in range(3):
        a[c][3] = summed1(c, 3)

    third_copies = {}
    for c, (axes, _, cols, rows, own_rows) in enumerate(COLOURS):
        total = a[c][3]
        for hop in HOPS:
            second_copies[c, hop].wait_recv()
            total = total + decoded(r2[c][hop - 1], sc2[c, hop - 1][0:1, 0:1] * unit)
        for w in range(4):
            b[c][w, pl.ds(0, own_rows), :] = total[w * own_rows : (w + 1) * own_rows]
        inv3 = (1.0 / sc3s[c])[0:1, 0:1]
        for hop in HOPS:
            w = (here[axes[2]] + hop) % 4
            q3[c][hop - 1, pl.ds(0, own_rows), :] = encoded(b[c][w, pl.ds(0, own_rows), :], inv3)
            copy = pltpu.make_async_remote_copy(
                src_ref=q3[c].at[hop - 1], dst_ref=r3[c].at[hop - 1],
                send_sem=send3.at[c, hop - 1], recv_sem=recv3.at[c, hop - 1],
                device_id=along(axes[2], hop), device_id_type=MESH,
            )
            copy.start()
            sent.append(copy)
            third_copies[c, hop] = copy

    for copy in scale3_copies:
        copy.wait_recv()
    for c, (axes, col, cols, _, _) in enumerate(COLOURS):
        total = b[c][here[axes[2]], pl.ds(0, 14), :]
        for hop in HOPS:
            third_copies[c, hop].wait_recv()
            scale = sc3[c, hop - 1][0:1, 0:1] * unit
            total = total + decoded(r3[c][hop - 1, pl.ds(0, 14), :], scale)
        o_ref[:, pl.ds(col, cols)] = total

    for copy in swaps + sent:
        copy.wait_send()


def on_device(factors, screen):
    f32, i16, bf16 = jnp.float32, jnp.int16, jnp.bfloat16
    v = pltpu.VMEM
    dma = pltpu.SemaphoreType.DMA
    per = [(c[2], c[3]) for c in COLOURS]
    scratch = [
        v((2 * DEPTH, NBF), bf16), v((704, 384), f32), v((4, 4, 56, DEPTH), f32),
        v((4, 224, 2 * DEPTH), bf16), v((4, 224, 2 * DEPTH), bf16), v((4, 4, 4, 16, 2 * DEPTH), bf16),
        v((4, 64, 640), f32),
        *[v((3, 4, rows, cols), i16) for cols, rows in per],
        *[v((3, 4, rows, cols), i16) for cols, rows in per],
        *[v((4, rows, cols), f32) for cols, rows in per],
        *[v((3, rows, cols), i16) for cols, rows in per],
        *[v((3, rows, cols), i16) for cols, rows in per],
        *[v((4, 16, cols), f32) for cols, rows in per],
        *[v((3, 16, cols), i16) for cols, rows in per],
        *[v((3, 16, cols), i16) for cols, rows in per],
        v((1, 18), jnp.int32), v((8, 128), f32), v((8, 128), f32), v((10, 8, 128), f32),
        v((3, 8, 128), f32), v((3, 3, 8, 128), f32), v((3, 8, 128), f32), v((3, 3, 8, 128), f32),
        dma((2,)), dma((4,)), dma((4,)), dma((3, 3, 4)), dma((3, 3, 4)), dma((3, 3)), dma((3, 3)),
        dma((3, 3)), dma((3, 3)), dma((9,)), dma((9,)), dma((3, 3)), dma((3, 3)), dma((3, 3)), dma((3, 3)),
    ]
    return pl.pallas_call(
        kernel,
        out_shape=jax.ShapeDtypeStruct((14, NBF), f32),
        in_specs=[pl.BlockSpec(memory_space=pl.ANY), pl.BlockSpec(memory_space=pltpu.VMEM)],
        out_specs=pl.BlockSpec(memory_space=pltpu.VMEM),
        scratch_shapes=scratch,
        compiler_params=pltpu.CompilerParams(
            collective_id=0, has_side_effects=True, vmem_limit_bytes=60 * 2**20
        ),
    )(factors, screen)


def solution(mesh):
    placed = (P(("grp", "mem"), None, None), P(("grp", "mem"), None))
    return jax.shard_map(
        on_device, mesh=mesh, in_specs=placed, out_specs=P(("grp", "mem"), None), check_vma=False
    )
```

```python
import jax
import jax.numpy as jnp
from jax import lax
from jax.experimental import pallas as pl
from jax.experimental.pallas import tpu as pltpu
from jax.sharding import PartitionSpec as P

MESH = pl.DeviceIdType.MESH
NBF = 1792
ROWS = 576
DEPTH = 640
CHUNK = 256
TOP = 32000.0
X, Y, Z = 0, 1, 2
COLOURS = (((X, Y, Z), 0, 640), ((Y, X, Z), 1280, 512), ((Z, Y, X), 640, 640))
HOPS = (1, 3, 2)
ALL = (1, 3, 2, 0)


def coded(value, inverse):
    level = lax.rsqrt(lax.rsqrt(jnp.abs(value) * inverse)) * TOP + 0.5
    code = level.astype(jnp.int32)
    return jnp.where(value < 0.0, -code, code)


def decoded(code, scale):
    level = code.astype(jnp.int32).astype(jnp.float32) * (1.0 / TOP)
    return level * jnp.abs(level) * (level * level) * scale


def power(exponent):
    return jnp.exp2(exponent)


def kernel(
    f_ref, s_ref, o_ref,
    fbuf, turned, order, g_rows, p_rows, w00, w01, w02, w03, w1, w20, w21, w22, w23,
    q10, q11, q12, r10, r11, r12,
    q20, q21, q22, r20, r21, r22, b0, b1, b2,
    own_screen, peer_screen, sc_own, sc_peer, mine_ref, sc1, exponents,
    load_sem, swap_send, swap_recv, send1, recv1, send2, recv2, ssend1, srecv1,
):
    q1, r1 = (q10, q11, q12), (r10, r11, r12)
    whole = ((w00, w01, w02, w03), w1, (w20, w21, w22, w23))
    q2, r2, b = (q20, q21, q22), (r20, r21, r22), (b0, b1, b2)
    grp, mem = lax.axis_index("grp"), lax.axis_index("mem")
    here = (mem // 4, grp // 2, mem % 4)
    core = grp % 2

    def at(axis, coordinate):
        place = list(here)
        place[axis] = coordinate
        return (place[Y] * 2 + core, place[X] * 4 + place[Z])

    def along(axis, hop):
        return at(axis, (here[axis] + hop) % 4)

    def remote(src, dst, send, recv, device):
        copy = pltpu.make_async_remote_copy(
            src_ref=src, dst_ref=dst, send_sem=send, recv_sem=recv, device_id=device, device_id_type=MESH
        )
        copy.start()
        sent.append(copy)
        return copy

    sent = []
    peer = (here[Y] * 2 + 1 - core, mem)
    barrier = pltpu.get_barrier_semaphore()
    pl.semaphore_signal(barrier, inc=1, device_id=peer, device_id_type=MESH)
    for axis in range(3):
        for hop in HOPS:
            pl.semaphore_signal(barrier, inc=1, device_id=along(axis, hop), device_id_type=MESH)
    loads = [
        pltpu.make_async_copy(f_ref.at[pl.ds(i * 144, 144)], fbuf.at[pl.ds(i * 144, 144)], load_sem.at[i])
        for i in range(4)
    ]
    loads.append(pltpu.make_async_copy(s_ref, own_screen, load_sem.at[4]))
    for load in loads:
        load.start()

    pl.semaphore_wait(barrier, 10)
    screen_swap = remote(s_ref, peer_screen, swap_send.at[7], swap_recv.at[7], peer)
    swaps = []

    def swap(i):
        columns = pl.ds(i * CHUNK, CHUNK)
        swaps.append(
            remote(
                fbuf.at[pl.ds(0, ROWS), columns],
                fbuf.at[pl.ds(DEPTH, ROWS), columns],
                swap_send.at[i], swap_recv.at[i], peer,
            )
        )

    for load in loads[:4]:
        load.wait()
    for i in range(4):
        swap(i)

    r = lax.broadcasted_iota(jnp.int32, (224, 224), 0).astype(jnp.float32)
    n = lax.broadcasted_iota(jnp.int32, (224, 224), 1).astype(jnp.float32)
    z = jnp.floor((r + 0.5) * (1.0 / 56.0))
    x = jnp.floor((r - z * 56.0 + 0.5) * (1.0 / 14.0))
    order[...] = jnp.where(r - z * 42.0 + x * 42.0 == n, 1.0, 0.0).astype(jnp.bfloat16)
    zero_rows = jnp.zeros((DEPTH - ROWS, NBF), jnp.bfloat16)
    fbuf[pl.ds(ROWS, DEPTH - ROWS), :] = zero_rows
    fbuf[pl.ds(DEPTH + ROWS, DEPTH - ROWS), :] = zero_rows
    kk = lax.broadcasted_iota(jnp.int32, (18, DEPTH), 1)
    jj = lax.broadcasted_iota(jnp.int32, (18, DEPTH), 0) * 16
    kk = jnp.where(kk >= 288, kk - 288, kk)
    spread = jnp.where((kk >= jj) & (kk < jj + 16), 1.0, 0.0).astype(jnp.bfloat16)

    def mask_of(ref):
        kept = jnp.where(ref[...] == 1, 1.0, 0.0).astype(jnp.bfloat16)
        kept = jnp.broadcast_to(kept, (16, 18))
        m = jnp.dot(kept, spread, preferred_element_type=jnp.float32)
        place = lax.broadcasted_iota(jnp.int32, (16, DEPTH), 1)
        return jnp.where(place < ROWS, m, 0.0).astype(jnp.bfloat16)

    def prepare(v, slot, first, mask):
        g = 2 * v + core
        tile = (224 * g) // 128 - g // 7
        off = 224 * g - 128 * tile
        window = fbuf[pl.ds(first, DEPTH), pl.ds(pl.multiple_of(tile * 128, 128), 384)]
        turned[slot] = window.T
        taken = turned[slot, pl.ds(pl.multiple_of(off, 32), 224), :] * mask[0:1]
        columns = pl.ds(first, DEPTH)
        g_rows[v, :, columns] = taken
        p_rows[v, :, columns] = jnp.dot(
            order[...], taken, preferred_element_type=jnp.float32
        ).astype(jnp.bfloat16)

    loads[4].wait()
    own_mask = mask_of(own_screen)
    own = fbuf[pl.ds(0, DEPTH), :]
    squares = jnp.dot(own_mask, own * own, preferred_element_type=jnp.float32)
    most = jnp.max(squares[0:8], axis=1, keepdims=True) * 1.02 + 1e-35
    sc_own[...] = jnp.broadcast_to(most, (8, 128))
    scale_swap = remote(sc_own, sc_peer, swap_send.at[8], swap_recv.at[8], peer)
    for i in range(4, 7):
        swap(i)
    for v in range(4):
        prepare(v, v, 0, own_mask)
    scale_swap.wait_recv()
    mine = sc_own[...] + sc_peer[...]
    mine_ref[...] = mine
    inverse = (1.0 / mine)[0:1, 0:1]
    scales1 = []
    for axis in range(3):
        for hop in HOPS:
            i = axis * 3 + hop - 1
            scales1.append(remote(mine_ref, sc1.at[i], ssend1.at[i], srecv1.at[i], along(axis, hop)))

    turns = [[(here[axes[1]] + hop) % 4 for hop in HOPS] + [here[axes[1]]] for axes, *_ in COLOURS]
    copies1 = {}

    def unit(c, j):
        _, col, cols = COLOURS[c]
        lhs = (g_rows if c == 0 else p_rows)[turns[c][j]]
        made = jnp.dot(lhs, fbuf[:, pl.ds(col, cols)], preferred_element_type=jnp.float32)
        whole[c][j][...] = made.reshape(4, 56, cols)

    def unit_by_place(hop):
        _, col, cols = COLOURS[1]
        lhs = g_rows[(here[Y] + hop) % 4]
        made = jnp.dot(lhs, fbuf[:, pl.ds(col, cols)], preferred_element_type=jnp.float32)
        whole[1][hop] = made.reshape(4, 56, cols)

    def emit(c, j):
        axis = COLOURS[c][0][0]
        for hop in HOPS:
            if c == 1:
                piece = whole[1][hop, turns[1][j]]
            else:
                piece = whole[c][j][(here[axis] + hop) % 4]
            q1[c][hop - 1, j] = coded(piece, inverse).astype(jnp.int16)
            copies1[c, j, hop] = remote(
                q1[c].at[hop - 1, j], r1[c].at[hop - 1, j], send1.at[c, hop - 1, j], recv1.at[c, hop - 1, j],
                along(axis, hop),
            )

    def first_sum(c, j):
        axis = COLOURS[c][0][0]
        total = whole[1][0, turns[1][j]] if c == 1 else whole[c][j][here[axis]]
        for hop in HOPS:
            copies1[c, j, hop].wait_recv()
            scale = sc1[axis * 3 + hop - 1][0:1, 0:1]
            total = total + decoded(r1[c][hop - 1, j], scale)
        return total

    def set_exponents():
        for copy in scales1:
            copy.wait_recv()
        for c, (axes, *_) in enumerate(COLOURS):
            i = axes[0] * 3
            bound = mine_ref[...] + sc1[i] + sc1[i + 1] + sc1[i + 2]
            exponents[c] = jnp.ceil(jnp.log(bound) * 1.4426950408889634 + 0.001)

    copies2 = {}

    def plane(c, j):
        axes, _, cols = COLOURS[c]
        total = first_sum(c, j)
        for w in range(4):
            b[c][j, w, 0:14, :] = total[w * 14 : w * 14 + 14]
        exponent = exponents[c][0:1, 0:1]
        inv = 1.0 / power(exponent)
        spare = exponent.astype(jnp.int32)
        row = lax.broadcasted_iota(jnp.int32, (16, cols), 0)
        hop2 = ALL[j]
        for k, hop3 in enumerate(ALL):
            if hop2 == 0 and hop3 == 0:
                continue
            w = (here[axes[2]] + hop3) % 4
            code = jnp.where(row < 14, coded(b[c][j, w], inv), spare)
            i = hop2 * 4 + hop3
            q2[c][i] = code.astype(jnp.int16)
            place = list(here)
            place[axes[1]] = turns[c][j]
            place[axes[2]] = w
            device = (place[Y] * 2 + core, place[X] * 4 + place[Z])
            copies2[c, i] = remote(q2[c].at[i], r2[c].at[i], send2.at[c, i], recv2.at[c, i], device)

    def last(c):
        axes, col, cols = COLOURS[c]
        total = b[c][3, here[axes[2]]]
        for hop2 in ALL:
            for hop3 in ALL:
                if hop2 == 0 and hop3 == 0:
                    continue
                i = hop2 * 4 + hop3
                copies2[c, i].wait_recv()
                code = r2[c][i].astype(jnp.int32)
                total = total + decoded(code, power(code[14:15].astype(jnp.float32)))
        o_ref[:, pl.ds(col, cols)] = total[0:14]

    landed = 0

    def land(upto):
        nonlocal landed
        while landed < upto:
            swaps[landed].wait_recv()
            landed += 1

    screen_swap.wait_recv()
    peer_mask = mask_of(peer_screen)
    land(7)
    along_y = turns[0]
    prepare(along_y[0], 0, DEPTH, peer_mask)
    unit(2, 0)
    emit(2, 0)
    unit(0, 0)
    emit(0, 0)
    prepare(along_y[1], 1, DEPTH, peer_mask)
    prepare(along_y[2], 2, DEPTH, peer_mask)
    unit_by_place(1)
    unit_by_place(3)
    unit_by_place(2)
    emit(1, 0)
    unit(2, 1)
    emit(1, 1)
    unit(0, 1)
    emit(2, 1)
    set_exponents()
    unit(2, 2)
    emit(0, 1)
    emit(1, 2)
    prepare(along_y[3], 3, DEPTH, peer_mask)
    unit(0, 2)
    emit(2, 2)
    emit(1, 3)
    unit(2, 3)
    emit(0, 2)
    unit(0, 3)
    emit(2, 3)
    unit_by_place(0)
    emit(0, 3)
    plane(0, 0)
    plane(1, 0)
    plane(2, 0)
    plane(0, 1)
    plane(1, 1)
    plane(2, 1)
    plane(1, 2)
    plane(0, 2)
    plane(2, 2)
    plane(1, 3)
    plane(0, 3)
    plane(2, 3)
    for copy in sent[:-45]:
        copy.wait_send()
    last(1)
    last(0)
    last(2)
    for copy in sent[-45:]:
        copy.wait_send()


def on_device(factors, screen):
    f32, i16, bf16 = jnp.float32, jnp.int16, jnp.bfloat16
    v = pltpu.VMEM
    dma = pltpu.SemaphoreType.DMA
    widths = [c[2] for c in COLOURS]

    def each(shape, dtype):
        return [v((*shape, w), dtype) for w in widths]

    scratch = [
        v((2 * DEPTH, NBF), bf16), v((4, 384, DEPTH), bf16), v((224, 224), bf16),
        v((4, 224, 2 * DEPTH), bf16), v((4, 224, 2 * DEPTH), bf16), *[v((4, 56, widths[0]), f32)] * 4,
        v((4, 4, 56, widths[1]), f32), *[v((4, 56, widths[2]), f32)] * 4,
        *each((3, 4, 56), i16), *each((3, 4, 56), i16),
        *each((16, 16), i16), *each((16, 16), i16), *each((4, 4, 16), f32),
        v((1, 18), jnp.int32), v((1, 18), jnp.int32), v((8, 128), f32), v((8, 128), f32), v((8, 128), f32),
        v((9, 8, 128), f32), v((3, 8, 128), f32),
        dma((5,)), dma((9,)), dma((9,)), dma((3, 3, 4)), dma((3, 3, 4)), dma((3, 16)), dma((3, 16)),
        dma((9,)), dma((9,)),
    ]
    return pl.pallas_call(
        kernel,
        out_shape=jax.ShapeDtypeStruct((14, NBF), f32),
        in_specs=[pl.BlockSpec(memory_space=pl.ANY)] * 2,
        out_specs=pl.BlockSpec(memory_space=pltpu.VMEM),
        scratch_shapes=scratch,
        compiler_params=pltpu.CompilerParams(
            collective_id=0, has_side_effects=True, vmem_limit_bytes=60 * 2**20
        ),
    )(factors.reshape(ROWS, NBF), screen)


def solution(mesh):
    placed = (P(("grp", "mem"), None, None), P(("grp", "mem"), None))
    return jax.shard_map(
        on_device, mesh=mesh, in_specs=placed, out_specs=P(("grp", "mem"), None), check_vma=False
    )
```

```python
import jax
import jax.numpy as jnp
from jax import lax
from jax.experimental import pallas as pl
from jax.experimental.pallas import tpu as pltpu
from jax.sharding import PartitionSpec as P

MESH = pl.DeviceIdType.MESH
NBF = 1792
ROWS = 576
DEPTH = 640
CHUNK = 256
TOP = 32000.0
X, Y, Z = 0, 1, 2
COLOURS = (((X, Y, Z), 0, 640), ((Y, X, Z), 1280, 512), ((Z, Y, X), 640, 640))
HOPS = (1, 3, 2)
ALL = (1, 3, 2, 0)


def coded(value, inverse):
    level = lax.rsqrt(lax.rsqrt(jnp.abs(value) * inverse)) * TOP + 0.5
    code = level.astype(jnp.int32)
    return jnp.where(value < 0.0, -code, code)


def decoded(code, scale):
    level = code.astype(jnp.int32).astype(jnp.float32) * (1.0 / TOP)
    return level * jnp.abs(level) * (level * level) * scale


def power(exponent):
    return jnp.exp2(exponent)


def kernel(
    f_ref, s_ref, o_ref,
    fbuf, turned, order, g_rows, p_rows, w00, w01, w02, w03, w1, w20, w21, w22, w23,
    q10, q11, q12, r10, r11, r12,
    q20, q21, q22, r20, r21, r22, b0, b1, b2,
    own_screen, peer_screen, sc_own, sc_peer, mine_ref, sc1, exponents,
    load_sem, swap_send, swap_recv, send1, recv1, send2, recv2, ssend1, srecv1,
):
    q1, r1 = (q10, q11, q12), (r10, r11, r12)
    whole = ((w00, w01, w02, w03), w1, (w20, w21, w22, w23))
    q2, r2, b = (q20, q21, q22), (r20, r21, r22), (b0, b1, b2)
    grp, mem = lax.axis_index("grp"), lax.axis_index("mem")
    here = (mem // 4, grp // 2, mem % 4)
    core = grp % 2

    def at(axis, coordinate):
        place = list(here)
        place[axis] = coordinate
        return (place[Y] * 2 + core, place[X] * 4 + place[Z])

    def along(axis, hop):
        return at(axis, (here[axis] + hop) % 4)

    def remote(src, dst, send, recv, device):
        copy = pltpu.make_async_remote_copy(
            src_ref=src, dst_ref=dst, send_sem=send, recv_sem=recv, device_id=device, device_id_type=MESH
        )
        copy.start()
        sent.append(copy)
        return copy

    sent = []
    peer = (here[Y] * 2 + 1 - core, mem)
    barrier = pltpu.get_barrier_semaphore()
    pl.semaphore_signal(barrier, inc=1, device_id=peer, device_id_type=MESH)
    for axis in range(3):
        for hop in HOPS:
            pl.semaphore_signal(barrier, inc=1, device_id=along(axis, hop), device_id_type=MESH)
    loads = [
        pltpu.make_async_copy(f_ref.at[pl.ds(i * 144, 144)], fbuf.at[pl.ds(i * 144, 144)], load_sem.at[i])
        for i in range(4)
    ]
    loads.append(pltpu.make_async_copy(s_ref, own_screen, load_sem.at[4]))
    for load in loads:
        load.start()

    pl.semaphore_wait(barrier, 10)
    screen_swap = remote(s_ref, peer_screen, swap_send.at[7], swap_recv.at[7], peer)
    swaps = []

    def swap(i):
        columns = pl.ds(i * CHUNK, CHUNK)
        swaps.append(
            remote(
                fbuf.at[pl.ds(0, ROWS), columns],
                fbuf.at[pl.ds(DEPTH, ROWS), columns],
                swap_send.at[i], swap_recv.at[i], peer,
            )
        )

    for load in loads[:4]:
        load.wait()
    for i in range(4):
        swap(i)

    r = lax.broadcasted_iota(jnp.int32, (224, 224), 0).astype(jnp.float32)
    n = lax.broadcasted_iota(jnp.int32, (224, 224), 1).astype(jnp.float32)
    z = jnp.floor((r + 0.5) * (1.0 / 56.0))
    x = jnp.floor((r - z * 56.0 + 0.5) * (1.0 / 14.0))
    order[...] = jnp.where(r - z * 42.0 + x * 42.0 == n, 1.0, 0.0).astype(jnp.bfloat16)
    zero_rows = jnp.zeros((DEPTH - ROWS, NBF), jnp.bfloat16)
    fbuf[pl.ds(ROWS, DEPTH - ROWS), :] = zero_rows
    fbuf[pl.ds(DEPTH + ROWS, DEPTH - ROWS), :] = zero_rows
    kk = lax.broadcasted_iota(jnp.int32, (18, DEPTH), 1)
    jj = lax.broadcasted_iota(jnp.int32, (18, DEPTH), 0) * 16
    kk = jnp.where(kk >= 288, kk - 288, kk)
    spread = jnp.where((kk >= jj) & (kk < jj + 16), 1.0, 0.0).astype(jnp.bfloat16)

    def mask_of(ref):
        kept = jnp.where(ref[...] == 1, 1.0, 0.0).astype(jnp.bfloat16)
        kept = jnp.broadcast_to(kept, (16, 18))
        m = jnp.dot(kept, spread, preferred_element_type=jnp.float32)
        place = lax.broadcasted_iota(jnp.int32, (16, DEPTH), 1)
        return jnp.where(place < ROWS, m, 0.0).astype(jnp.bfloat16)

    def prepare(v, slot, first, mask):
        g = 2 * v + core
        tile = (224 * g) // 128 - g // 7
        off = 224 * g - 128 * tile
        window = fbuf[pl.ds(first, DEPTH), pl.ds(pl.multiple_of(tile * 128, 128), 384)]
        turned[slot] = window.T
        taken = turned[slot, pl.ds(pl.multiple_of(off, 32), 224), :] * mask[0:1]
        columns = pl.ds(first, DEPTH)
        g_rows[v, :, columns] = taken
        p_rows[v, :, columns] = jnp.dot(
            order[...], taken, preferred_element_type=jnp.float32
        ).astype(jnp.bfloat16)

    loads[4].wait()
    own_mask = mask_of(own_screen)
    own = fbuf[pl.ds(0, DEPTH), :]
    squares = jnp.dot(own_mask, own * own, preferred_element_type=jnp.float32)
    most = jnp.max(squares[0:8], axis=1, keepdims=True) * 1.02 + 1e-35
    sc_own[...] = jnp.broadcast_to(most, (8, 128))
    scale_swap = remote(sc_own, sc_peer, swap_send.at[8], swap_recv.at[8], peer)
    for i in range(4, 7):
        swap(i)
    for v in range(4):
        prepare(v, v, 0, own_mask)
    scale_swap.wait_recv()
    mine = sc_own[...] + sc_peer[...]
    mine_ref[...] = mine
    inverse = (1.0 / mine)[0:1, 0:1]
    scales1 = []
    for axis in range(3):
        for hop in HOPS:
            i = axis * 3 + hop - 1
            scales1.append(remote(mine_ref, sc1.at[i], ssend1.at[i], srecv1.at[i], along(axis, hop)))

    turns = [[(here[axes[1]] + hop) % 4 for hop in HOPS] + [here[axes[1]]] for axes, *_ in COLOURS]
    copies1 = {}

    def unit(c, j):
        _, col, cols = COLOURS[c]
        lhs = (g_rows if c == 0 else p_rows)[turns[c][j]]
        made = jnp.dot(lhs, fbuf[:, pl.ds(col, cols)], preferred_element_type=jnp.float32)
        whole[c][j][...] = made.reshape(4, 56, cols)

    def unit_by_place(hop):
        _, col, cols = COLOURS[1]
        lhs = g_rows[(here[Y] + hop) % 4]
        made = jnp.dot(lhs, fbuf[:, pl.ds(col, cols)], preferred_element_type=jnp.float32)
        whole[1][hop] = made.reshape(4, 56, cols)

    def emit(c, j):
        axis = COLOURS[c][0][0]
        for hop in HOPS:
            if c == 1:
                piece = whole[1][hop, turns[1][j]]
            else:
                piece = whole[c][j][(here[axis] + hop) % 4]
            q1[c][hop - 1, j] = coded(piece, inverse).astype(jnp.int16)
            copies1[c, j, hop] = remote(
                q1[c].at[hop - 1, j], r1[c].at[hop - 1, j], send1.at[c, hop - 1, j], recv1.at[c, hop - 1, j],
                along(axis, hop),
            )

    def first_sum(c, j):
        axis = COLOURS[c][0][0]
        total = whole[1][0, turns[1][j]] if c == 1 else whole[c][j][here[axis]]
        for hop in HOPS:
            copies1[c, j, hop].wait_recv()
            scale = sc1[axis * 3 + hop - 1][0:1, 0:1]
            total = total + decoded(r1[c][hop - 1, j], scale)
        return total

    def set_exponents():
        for copy in scales1:
            copy.wait_recv()
        for c, (axes, *_) in enumerate(COLOURS):
            i = axes[0] * 3
            bound = mine_ref[...] + sc1[i] + sc1[i + 1] + sc1[i + 2]
            exponents[c] = jnp.ceil(jnp.log(bound) * 1.4426950408889634 + 0.001)

    copies2 = {}

    def plane(c, j):
        axes, _, cols = COLOURS[c]
        total = first_sum(c, j)
        for w in range(4):
            b[c][j, w, 0:14, :] = total[w * 14 : w * 14 + 14]
        exponent = exponents[c][0:1, 0:1]
        inv = 1.0 / power(exponent)
        spare = exponent.astype(jnp.int32)
        row = lax.broadcasted_iota(jnp.int32, (16, cols), 0)
        hop2 = ALL[j]
        for k, hop3 in enumerate(ALL):
            if hop2 == 0 and hop3 == 0:
                continue
            w = (here[axes[2]] + hop3) % 4
            code = jnp.where(row < 14, coded(b[c][j, w], inv), spare)
            i = hop2 * 4 + hop3
            q2[c][i] = code.astype(jnp.int16)
            place = list(here)
            place[axes[1]] = turns[c][j]
            place[axes[2]] = w
            device = (place[Y] * 2 + core, place[X] * 4 + place[Z])
            copies2[c, i] = remote(q2[c].at[i], r2[c].at[i], send2.at[c, i], recv2.at[c, i], device)

    def last(c):
        axes, col, cols = COLOURS[c]
        total = b[c][3, here[axes[2]]]
        for hop2 in ALL:
            for hop3 in ALL:
                if hop2 == 0 and hop3 == 0:
                    continue
                i = hop2 * 4 + hop3
                copies2[c, i].wait_recv()
                code = r2[c][i].astype(jnp.int32)
                total = total + decoded(code, power(code[14:15].astype(jnp.float32)))
        o_ref[:, pl.ds(col, cols)] = total[0:14]

    landed = 0

    def land(upto):
        nonlocal landed
        while landed < upto:
            swaps[landed].wait_recv()
            landed += 1

    screen_swap.wait_recv()
    peer_mask = mask_of(peer_screen)
    land(7)
    along_y = turns[0]
    prepare(along_y[0], 0, DEPTH, peer_mask)
    unit(2, 0)
    emit(2, 0)
    unit(0, 0)
    emit(0, 0)
    prepare(along_y[1], 1, DEPTH, peer_mask)
    prepare(along_y[2], 2, DEPTH, peer_mask)
    unit_by_place(1)
    unit_by_place(3)
    unit_by_place(2)
    emit(1, 0)
    unit(2, 1)
    emit(1, 1)
    unit(0, 1)
    emit(2, 1)
    set_exponents()
    unit(2, 2)
    emit(0, 1)
    emit(1, 2)
    prepare(along_y[3], 3, DEPTH, peer_mask)
    unit(0, 2)
    emit(2, 2)
    emit(1, 3)
    unit(2, 3)
    emit(0, 2)
    unit(0, 3)
    emit(2, 3)
    unit_by_place(0)
    emit(0, 3)
    plane(0, 0)
    plane(1, 0)
    plane(2, 0)
    plane(0, 1)
    plane(1, 1)
    plane(2, 1)
    plane(1, 2)
    plane(0, 2)
    plane(2, 2)
    plane(1, 3)
    plane(0, 3)
    plane(2, 3)
    for copy in sent[:-45]:
        copy.wait_send()
    last(1)
    last(0)
    last(2)
    for copy in sent[-45:]:
        copy.wait_send()


def on_device(factors, screen):
    f32, i16, bf16 = jnp.float32, jnp.int16, jnp.bfloat16
    v = pltpu.VMEM
    dma = pltpu.SemaphoreType.DMA
    widths = [c[2] for c in COLOURS]

    def each(shape, dtype):
        return [v((*shape, w), dtype) for w in widths]

    scratch = [
        v((2 * DEPTH, NBF), bf16), v((4, 384, DEPTH), bf16), v((224, 224), bf16),
        v((4, 224, 2 * DEPTH), bf16), v((4, 224, 2 * DEPTH), bf16), *[v((4, 56, widths[0]), f32)] * 4,
        v((4, 4, 56, widths[1]), f32), *[v((4, 56, widths[2]), f32)] * 4,
        *each((3, 4, 56), i16), *each((3, 4, 56), i16),
        *each((16, 16), i16), *each((16, 16), i16), *each((4, 4, 16), f32),
        v((1, 18), jnp.int32), v((1, 18), jnp.int32), v((8, 128), f32), v((8, 128), f32), v((8, 128), f32),
        v((9, 8, 128), f32), v((3, 8, 128), f32),
        dma((5,)), dma((9,)), dma((9,)), dma((3, 3, 4)), dma((3, 3, 4)), dma((3, 16)), dma((3, 16)),
        dma((9,)), dma((9,)),
    ]
    return pl.pallas_call(
        kernel,
        out_shape=jax.ShapeDtypeStruct((14, NBF), f32),
        in_specs=[pl.BlockSpec(memory_space=pltpu.HBM)] * 2,
        out_specs=pl.BlockSpec(memory_space=pltpu.VMEM),
        scratch_shapes=scratch,
        compiler_params=pltpu.CompilerParams(
            collective_id=0, has_side_effects=True, vmem_limit_bytes=55000000
        ),
    )(factors.reshape(ROWS, NBF), screen)


def solution(mesh):
    placed = (P(("grp", "mem"), None, None), P(("grp", "mem"), None))
    return jax.shard_map(
        on_device, mesh=mesh, in_specs=placed, out_specs=P(("grp", "mem"), None), check_vma=False
    )
```

```python
import jax
import jax.numpy as jnp
from jax import lax
from jax.experimental import pallas as pl
from jax.experimental.pallas import tpu as pltpu
from jax.sharding import PartitionSpec as P

MESH = pl.DeviceIdType.MESH
NBF = 1792
ROWS = 576
DEPTH = 640
CHUNK = 144
TOP = 32000.0
X, Y, Z = 0, 1, 2
COLOURS = (((X, Y, Z), 0, 640), ((Y, X, Z), 1280, 512), ((Z, Y, X), 640, 640))
HOPS = (1, 3, 2)
ALL = (1, 3, 2, 0)


def coded(value, inverse):
    level = lax.rsqrt(lax.rsqrt(jnp.abs(value) * inverse)) * TOP + 0.5
    code = level.astype(jnp.int32)
    return jnp.where(value < 0.0, -code, code)


def decoded(code, scale):
    level = code.astype(jnp.int32).astype(jnp.float32) * (1.0 / TOP)
    return level * jnp.abs(level) * (level * level) * scale


def power(exponent):
    return jnp.exp2(exponent)


def kernel(
    f_ref, s_ref, o_ref,
    fbuf, turned, order, g_rows, p_rows, w00, w01, w02, w03, w1, w20, w21, w22, w23,
    q10, q11, q12, r10, r11, r12,
    q20, q21, q22, r20, r21, r22, b0, b1, b2,
    own_screen, peer_screen, sc_own, sc_peer, mine_ref, sc1, exponents,
    load_sem, swap_send, swap_recv, send1, recv1, send2, recv2, ssend1, srecv1,
):
    q1, r1 = (q10, q11, q12), (r10, r11, r12)
    whole = ((w00, w01, w02, w03), w1, (w20, w21, w22, w23))
    q2, r2, b = (q20, q21, q22), (r20, r21, r22), (b0, b1, b2)
    grp, mem = lax.axis_index("grp"), lax.axis_index("mem")
    here = (mem // 4, grp // 2, mem % 4)
    core = grp % 2

    def at(axis, coordinate):
        place = list(here)
        place[axis] = coordinate
        return (place[Y] * 2 + core, place[X] * 4 + place[Z])

    def along(axis, hop):
        return at(axis, (here[axis] + hop) % 4)

    def remote(src, dst, send, recv, device):
        copy = pltpu.make_async_remote_copy(
            src_ref=src, dst_ref=dst, send_sem=send, recv_sem=recv, device_id=device, device_id_type=MESH
        )
        copy.start()
        sent.append(copy)
        return copy

    sent = []
    peer = (here[Y] * 2 + 1 - core, mem)
    barrier = pltpu.get_barrier_semaphore()
    pl.semaphore_signal(barrier, inc=1, device_id=peer, device_id_type=MESH)
    for axis in range(3):
        for hop in HOPS:
            pl.semaphore_signal(barrier, inc=1, device_id=along(axis, hop), device_id_type=MESH)
    loads = [
        pltpu.make_async_copy(f_ref.at[pl.ds(i * 144, 144)], fbuf.at[pl.ds(i * 144, 144)], load_sem.at[i])
        for i in range(4)
    ]
    loads.append(pltpu.make_async_copy(s_ref, own_screen, load_sem.at[4]))
    for load in loads:
        load.start()

    pl.semaphore_wait(barrier, 10)
    screen_swap = remote(s_ref, peer_screen, swap_send.at[7], swap_recv.at[7], peer)
    swaps = []

    def swap(i):
        swaps.append(
            remote(
                fbuf.at[pl.ds(i * CHUNK, CHUNK)], fbuf.at[pl.ds(DEPTH + i * CHUNK, CHUNK)],
                swap_send.at[i], swap_recv.at[i], peer,
            )
        )

    for load in loads[:4]:
        load.wait()
    for i in range(2):
        swap(i)

    r = lax.broadcasted_iota(jnp.int32, (224, 224), 0).astype(jnp.float32)
    n = lax.broadcasted_iota(jnp.int32, (224, 224), 1).astype(jnp.float32)
    z = jnp.floor((r + 0.5) * (1.0 / 56.0))
    x = jnp.floor((r - z * 56.0 + 0.5) * (1.0 / 14.0))
    order[...] = jnp.where(r - z * 42.0 + x * 42.0 == n, 1.0, 0.0).astype(jnp.bfloat16)
    zero_rows = jnp.zeros((DEPTH - ROWS, NBF), jnp.bfloat16)
    fbuf[pl.ds(ROWS, DEPTH - ROWS), :] = zero_rows
    fbuf[pl.ds(DEPTH + ROWS, DEPTH - ROWS), :] = zero_rows
    kk = lax.broadcasted_iota(jnp.int32, (18, DEPTH), 1)
    jj = lax.broadcasted_iota(jnp.int32, (18, DEPTH), 0) * 16
    kk = jnp.where(kk >= 288, kk - 288, kk)
    spread = jnp.where((kk >= jj) & (kk < jj + 16), 1.0, 0.0).astype(jnp.bfloat16)

    def mask_of(ref):
        kept = jnp.where(ref[...] == 1, 1.0, 0.0).astype(jnp.bfloat16)
        kept = jnp.broadcast_to(kept, (16, 18))
        m = jnp.dot(kept, spread, preferred_element_type=jnp.float32)
        place = lax.broadcasted_iota(jnp.int32, (16, DEPTH), 1)
        return jnp.where(place < ROWS, m, 0.0).astype(jnp.bfloat16)

    def prepare(v, slot, first, mask):
        g = 2 * v + core
        tile = (224 * g) // 128 - g // 7
        off = 224 * g - 128 * tile
        window = fbuf[pl.ds(first, DEPTH), pl.ds(pl.multiple_of(tile * 128, 128), 384)]
        turned[slot] = window.T
        taken = turned[slot, pl.ds(pl.multiple_of(off, 32), 224), :] * mask[0:1]
        columns = pl.ds(first, DEPTH)
        g_rows[v, :, columns] = taken
        p_rows[v, :, columns] = jnp.dot(
            order[...], taken, preferred_element_type=jnp.float32
        ).astype(jnp.bfloat16)

    loads[4].wait()
    own_mask = mask_of(own_screen)
    own = fbuf[pl.ds(0, DEPTH), :]
    squares = jnp.dot(own_mask, own * own, preferred_element_type=jnp.float32)
    most = jnp.max(squares[0:8], axis=1, keepdims=True) * 1.02 + 1e-35
    sc_own[...] = jnp.broadcast_to(most, (8, 128))
    scale_swap = remote(sc_own, sc_peer, swap_send.at[8], swap_recv.at[8], peer)
    for i in range(2, 4):
        swap(i)
    for v in range(4):
        prepare(v, v, 0, own_mask)
    scale_swap.wait_recv()
    mine = sc_own[...] + sc_peer[...]
    mine_ref[...] = mine
    inverse = (1.0 / mine)[0:1, 0:1]
    scales1 = []
    for axis in range(3):
        for hop in HOPS:
            i = axis * 3 + hop - 1
            scales1.append(remote(mine_ref, sc1.at[i], ssend1.at[i], srecv1.at[i], along(axis, hop)))

    turns = [[(here[axes[1]] + hop) % 4 for hop in HOPS] + [here[axes[1]]] for axes, *_ in COLOURS]
    copies1 = {}

    def unit(c, j):
        _, col, cols = COLOURS[c]
        lhs = (g_rows if c == 0 else p_rows)[turns[c][j]]
        made = jnp.dot(lhs, fbuf[:, pl.ds(col, cols)], preferred_element_type=jnp.float32)
        whole[c][j][...] = made.reshape(4, 56, cols)

    def unit_by_place(hop):
        _, col, cols = COLOURS[1]
        lhs = g_rows[(here[Y] + hop) % 4]
        made = jnp.dot(lhs, fbuf[:, pl.ds(col, cols)], preferred_element_type=jnp.float32)
        whole[1][hop] = made.reshape(4, 56, cols)

    def emit(c, j):
        axis = COLOURS[c][0][0]
        for hop in (2, 1, 3):
            if c == 1:
                piece = whole[1][hop, turns[1][j]]
            else:
                piece = whole[c][j][(here[axis] + hop) % 4]
            q1[c][hop - 1, j] = coded(piece, inverse).astype(jnp.int16)
            copies1[c, j, hop] = remote(
                q1[c].at[hop - 1, j], r1[c].at[hop - 1, j], send1.at[c, hop - 1, j], recv1.at[c, hop - 1, j],
                along(axis, hop),
            )

    def first_sum(c, j):
        axis = COLOURS[c][0][0]
        total = whole[1][0, turns[1][j]] if c == 1 else whole[c][j][here[axis]]
        for hop in HOPS:
            copies1[c, j, hop].wait_recv()
            scale = sc1[axis * 3 + hop - 1][0:1, 0:1]
            total = total + decoded(r1[c][hop - 1, j], scale)
        return total

    def set_exponents():
        for copy in scales1:
            copy.wait_recv()
        for c, (axes, *_) in enumerate(COLOURS):
            i = axes[0] * 3
            bound = mine_ref[...] + sc1[i] + sc1[i + 1] + sc1[i + 2]
            exponents[c] = jnp.ceil(jnp.log(bound) * 1.4426950408889634 + 0.001)

    copies2 = {}

    def plane(c, j):
        axes, _, cols = COLOURS[c]
        total = first_sum(c, j)
        for w in range(4):
            b[c][j, w, 0:14, :] = total[w * 14 : w * 14 + 14]
        exponent = exponents[c][0:1, 0:1]
        inv = 1.0 / power(exponent)
        spare = exponent.astype(jnp.int32)
        row = lax.broadcasted_iota(jnp.int32, (16, cols), 0)
        hop2 = ALL[j]
        for k, hop3 in enumerate((2, 1, 3, 0)):
            if hop2 == 0 and hop3 == 0:
                continue
            w = (here[axes[2]] + hop3) % 4
            code = jnp.where(row < 14, coded(b[c][j, w], inv), spare)
            i = hop2 * 4 + hop3
            q2[c][i] = code.astype(jnp.int16)
            place = list(here)
            place[axes[1]] = turns[c][j]
            place[axes[2]] = w
            device = (place[Y] * 2 + core, place[X] * 4 + place[Z])
            copies2[c, i] = remote(q2[c].at[i], r2[c].at[i], send2.at[c, i], recv2.at[c, i], device)

    def last(c):
        axes, col, cols = COLOURS[c]
        total = b[c][3, here[axes[2]]]
        for hop2 in ALL:
            for hop3 in ALL:
                if hop2 == 0 and hop3 == 0:
                    continue
                i = hop2 * 4 + hop3
                copies2[c, i].wait_recv()
                code = r2[c][i].astype(jnp.int32)
                total = total + decoded(code, power(code[14:15].astype(jnp.float32)))
        o_ref[:, pl.ds(col, cols)] = total[0:14]

    landed = 0

    def land(upto):
        nonlocal landed
        while landed < upto:
            swaps[landed].wait_recv()
            landed += 1

    screen_swap.wait_recv()
    peer_mask = mask_of(peer_screen)
    land(4)
    along_y = turns[0]
    prepare(along_y[0], 0, DEPTH, peer_mask)
    unit(2, 0)
    emit(2, 0)
    unit(0, 0)
    emit(0, 0)
    prepare(along_y[1], 1, DEPTH, peer_mask)
    prepare(along_y[2], 2, DEPTH, peer_mask)
    unit_by_place(1)
    unit_by_place(3)
    unit_by_place(2)
    emit(1, 0)
    unit(2, 1)
    emit(1, 1)
    unit(0, 1)
    emit(2, 1)
    set_exponents()
    unit(2, 2)
    emit(0, 1)
    emit(1, 2)
    prepare(along_y[3], 3, DEPTH, peer_mask)
    unit(0, 2)
    emit(2, 2)
    emit(1, 3)
    plane(2, 0)
    unit(2, 3)
    emit(0, 2)
    plane(0, 0)
    unit(0, 3)
    emit(2, 3)
    unit_by_place(0)
    emit(0, 3)
    plane(1, 0)
    plane(0, 1)
    plane(1, 1)
    plane(2, 1)
    plane(1, 2)
    plane(0, 2)
    plane(2, 2)
    plane(1, 3)
    plane(0, 3)
    plane(2, 3)
    for copy in sent[:-45]:
        copy.wait_send()
    last(1)
    last(0)
    last(2)
    for copy in sent[-45:]:
        copy.wait_send()


def on_device(factors, screen):
    f32, i16, bf16 = jnp.float32, jnp.int16, jnp.bfloat16
    v = pltpu.VMEM
    dma = pltpu.SemaphoreType.DMA
    widths = [c[2] for c in COLOURS]

    def each(shape, dtype):
        return [v((*shape, w), dtype) for w in widths]

    scratch = [
        v((2 * DEPTH, NBF), bf16), v((4, 384, DEPTH), bf16), v((224, 224), bf16),
        v((4, 224, 2 * DEPTH), bf16), v((4, 224, 2 * DEPTH), bf16), *[v((4, 56, widths[0]), f32)] * 4,
        v((4, 4, 56, widths[1]), f32), *[v((4, 56, widths[2]), f32)] * 4,
        *each((3, 4, 56), i16), *each((3, 4, 56), i16),
        *each((16, 16), i16), *each((16, 16), i16), *each((4, 4, 16), f32),
        v((1, 18), jnp.int32), v((1, 18), jnp.int32), v((8, 128), f32), v((8, 128), f32), v((8, 128), f32),
        v((9, 8, 128), f32), v((3, 8, 128), f32),
        dma((5,)), dma((9,)), dma((9,)), dma((3, 3, 4)), dma((3, 3, 4)), dma((3, 16)), dma((3, 16)),
        dma((9,)), dma((9,)),
    ]
    return pl.pallas_call(
        kernel,
        out_shape=jax.ShapeDtypeStruct((14, NBF), f32),
        in_specs=[pl.BlockSpec(memory_space=pltpu.HBM)] * 2,
        out_specs=pl.BlockSpec(memory_space=pltpu.VMEM),
        scratch_shapes=scratch,
        compiler_params=pltpu.CompilerParams(
            collective_id=0, has_side_effects=True, vmem_limit_bytes=55000000
        ),
    )(factors.reshape(ROWS, NBF), screen)


def solution(mesh):
    placed = (P(("grp", "mem"), None, None), P(("grp", "mem"), None))
    return jax.shard_map(
        on_device, mesh=mesh, in_specs=placed, out_specs=P(("grp", "mem"), None), check_vma=False
    )
```

```python
import jax
import jax.numpy as jnp
from jax import lax
from jax.experimental import pallas as pl
from jax.experimental.pallas import tpu as pltpu
from jax.sharding import PartitionSpec as P

MESH = pl.DeviceIdType.MESH
NBF = 1792
ROWS = 576
DEPTH = 640
CHUNK = 144
TOP = 32000.0
X, Y, Z = 0, 1, 2
COLOURS = (((X, Y, Z), 0, 640), ((Y, X, Z), 1280, 512), ((Z, Y, X), 640, 640))
HOPS = (1, 3, 2)
ALL = (1, 3, 2, 0)


def coded(value, inverse):
    level = lax.rsqrt(lax.rsqrt(jnp.abs(value) * inverse)) * TOP + 0.5
    code = level.astype(jnp.int32)
    return jnp.where(value < 0.0, -code, code)


def decoded(code, scale):
    level = code.astype(jnp.int32).astype(jnp.float32) * (1.0 / TOP)
    return level * jnp.abs(level) * (level * level) * scale


def power(exponent):
    return jnp.exp2(exponent)


def kernel(
    f_ref, s_ref, o_ref,
    fbuf, turned, order, g_rows, p_rows, w00, w01, w02, w03, w1, w20, w21, w22, w23,
    q10, q11, q12, r10, r11, r12,
    q20, q21, q22, r20, r21, r22, b0, b1, b2,
    own_screen, peer_screen, sc_own, sc_peer, mine_ref, sc1, exponents,
    load_sem, swap_send, swap_recv, send1, recv1, send2, recv2, ssend1, srecv1,
):
    q1, r1 = (q10, q11, q12), (r10, r11, r12)
    whole = ((w00, w01, w02, w03), w1, (w20, w21, w22, w23))
    q2, r2, b = (q20, q21, q22), (r20, r21, r22), (b0, b1, b2)
    grp, mem = lax.axis_index("grp"), lax.axis_index("mem")
    here = (mem // 4, grp // 2, mem % 4)
    core = grp % 2

    def at(axis, coordinate):
        place = list(here)
        place[axis] = coordinate
        return (place[Y] * 2 + core, place[X] * 4 + place[Z])

    def along(axis, hop):
        return at(axis, (here[axis] + hop) % 4)

    def remote(src, dst, send, recv, device):
        copy = pltpu.make_async_remote_copy(
            src_ref=src, dst_ref=dst, send_sem=send, recv_sem=recv, device_id=device, device_id_type=MESH
        )
        copy.start()
        sent.append(copy)
        return copy

    sent = []
    peer = (here[Y] * 2 + 1 - core, mem)
    barrier = pltpu.get_barrier_semaphore()
    pl.semaphore_signal(barrier, inc=1, device_id=peer, device_id_type=MESH)
    for axis in range(3):
        for hop in HOPS:
            pl.semaphore_signal(barrier, inc=1, device_id=along(axis, hop), device_id_type=MESH)
    loads = [
        pltpu.make_async_copy(f_ref.at[pl.ds(i * 144, 144)], fbuf.at[pl.ds(i * 144, 144)], load_sem.at[i])
        for i in range(4)
    ]
    loads.append(pltpu.make_async_copy(s_ref, own_screen, load_sem.at[4]))
    for load in loads:
        load.start()

    pl.semaphore_wait(barrier, 10)
    screen_swap = remote(s_ref, peer_screen, swap_send.at[7], swap_recv.at[7], peer)
    swaps = []

    def swap(i):
        swaps.append(
            remote(
                fbuf.at[pl.ds(i * CHUNK, CHUNK)], fbuf.at[pl.ds(DEPTH + i * CHUNK, CHUNK)],
                swap_send.at[i], swap_recv.at[i], peer,
            )
        )

    for load in loads[:4]:
        load.wait()
    for i in range(2):
        swap(i)

    r = lax.broadcasted_iota(jnp.int32, (224, 224), 0).astype(jnp.float32)
    n = lax.broadcasted_iota(jnp.int32, (224, 224), 1).astype(jnp.float32)
    z = jnp.floor((r + 0.5) * (1.0 / 56.0))
    x = jnp.floor((r - z * 56.0 + 0.5) * (1.0 / 14.0))
    order[...] = jnp.where(r - z * 42.0 + x * 42.0 == n, 1.0, 0.0).astype(jnp.bfloat16)
    zero_rows = jnp.zeros((DEPTH - ROWS, NBF), jnp.bfloat16)
    fbuf[pl.ds(ROWS, DEPTH - ROWS), :] = zero_rows
    fbuf[pl.ds(DEPTH + ROWS, DEPTH - ROWS), :] = zero_rows
    kk = lax.broadcasted_iota(jnp.int32, (18, DEPTH), 1)
    jj = lax.broadcasted_iota(jnp.int32, (18, DEPTH), 0) * 16
    kk = jnp.where(kk >= 288, kk - 288, kk)
    spread = jnp.where((kk >= jj) & (kk < jj + 16), 1.0, 0.0).astype(jnp.bfloat16)

    def mask_of(ref):
        kept = jnp.where(ref[...] == 1, 1.0, 0.0).astype(jnp.bfloat16)
        kept = jnp.broadcast_to(kept, (16, 18))
        m = jnp.dot(kept, spread, preferred_element_type=jnp.float32)
        place = lax.broadcasted_iota(jnp.int32, (16, DEPTH), 1)
        return jnp.where(place < ROWS, m, 0.0).astype(jnp.bfloat16)

    def prepare(v, slot, first, mask):
        g = 2 * v + core
        tile = (224 * g) // 128 - g // 7
        off = 224 * g - 128 * tile
        window = fbuf[pl.ds(first, DEPTH), pl.ds(pl.multiple_of(tile * 128, 128), 384)]
        turned[slot] = window.T
        taken = turned[slot, pl.ds(pl.multiple_of(off, 32), 224), :] * mask[0:1]
        columns = pl.ds(first, DEPTH)
        g_rows[v, :, columns] = taken
        p_rows[v, :, columns] = jnp.dot(
            order[...], taken, preferred_element_type=jnp.float32
        ).astype(jnp.bfloat16)

    loads[4].wait()
    own_mask = mask_of(own_screen)
    own = fbuf[pl.ds(0, DEPTH), :]
    squares = jnp.dot(own_mask, own * own, preferred_element_type=jnp.float32)
    most = jnp.max(squares[0:8], axis=1, keepdims=True) * 1.02 + 1e-35
    sc_own[...] = jnp.broadcast_to(most, (8, 128))
    scale_swap = remote(sc_own, sc_peer, swap_send.at[8], swap_recv.at[8], peer)
    for i in range(2, 4):
        swap(i)
    for v in range(4):
        prepare(v, v, 0, own_mask)
    scale_swap.wait_recv()
    mine = sc_own[...] + sc_peer[...]
    mine_ref[...] = mine
    inverse = (1.0 / mine)[0:1, 0:1]
    scales1 = []
    for axis in range(3):
        for hop in HOPS:
            i = axis * 3 + hop - 1
            scales1.append(remote(mine_ref, sc1.at[i], ssend1.at[i], srecv1.at[i], along(axis, hop)))

    turns = [[(here[axes[1]] + hop) % 4 for hop in HOPS] + [here[axes[1]]] for axes, *_ in COLOURS]
    copies1 = {}

    def unit(c, j):
        _, col, cols = COLOURS[c]
        lhs = (g_rows if c == 0 else p_rows)[turns[c][j]]
        made = jnp.dot(lhs, fbuf[:, pl.ds(col, cols)], preferred_element_type=jnp.float32)
        whole[c][j][...] = made.reshape(4, 56, cols)

    def unit_by_place(hop):
        _, col, cols = COLOURS[1]
        lhs = g_rows[(here[Y] + hop) % 4]
        made = jnp.dot(lhs, fbuf[:, pl.ds(col, cols)], preferred_element_type=jnp.float32)
        whole[1][hop] = made.reshape(4, 56, cols)

    def emit(c, j):
        axis = COLOURS[c][0][0]
        for hop in (2, 1, 3):
            if c == 1:
                piece = whole[1][hop, turns[1][j]]
            else:
                piece = whole[c][j][(here[axis] + hop) % 4]
            q1[c][hop - 1, j] = coded(piece, inverse).astype(jnp.int16)
            copies1[c, j, hop] = remote(
                q1[c].at[hop - 1, j], r1[c].at[hop - 1, j], send1.at[c, hop - 1, j], recv1.at[c, hop - 1, j],
                along(axis, hop),
            )

    def first_sum(c, j):
        axis = COLOURS[c][0][0]
        total = whole[1][0, turns[1][j]] if c == 1 else whole[c][j][here[axis]]
        for hop in HOPS:
            copies1[c, j, hop].wait_recv()
            scale = sc1[axis * 3 + hop - 1][0:1, 0:1]
            total = total + decoded(r1[c][hop - 1, j], scale)
        return total

    def set_exponents():
        for copy in scales1:
            copy.wait_recv()
        for c, (axes, *_) in enumerate(COLOURS):
            i = axes[0] * 3
            bound = mine_ref[...] + sc1[i] + sc1[i + 1] + sc1[i + 2]
            exponents[c] = jnp.ceil(jnp.log(bound) * 1.4426950408889634 + 0.001)

    copies2 = {}

    def plane(c, j):
        axes, _, cols = COLOURS[c]
        total = first_sum(c, j)
        for w in range(4):
            b[c][j, w, 0:14, :] = total[w * 14 : w * 14 + 14]
        exponent = exponents[c][0:1, 0:1]
        inv = 1.0 / power(exponent)
        spare = exponent.astype(jnp.int32)
        row = lax.broadcasted_iota(jnp.int32, (16, cols), 0)
        hop2 = ALL[j]
        for k, hop3 in enumerate((2, 1, 3, 0)):
            if hop2 == 0 and hop3 == 0:
                continue
            w = (here[axes[2]] + hop3) % 4
            code = jnp.where(row < 14, coded(b[c][j, w], inv), spare)
            i = hop2 * 4 + hop3
            q2[c][i] = code.astype(jnp.int16)
            place = list(here)
            place[axes[1]] = turns[c][j]
            place[axes[2]] = w
            device = (place[Y] * 2 + core, place[X] * 4 + place[Z])
            copies2[c, i] = remote(q2[c].at[i], r2[c].at[i], send2.at[c, i], recv2.at[c, i], device)

    def last(c):
        axes, col, cols = COLOURS[c]
        total = b[c][3, here[axes[2]]]
        for hop2 in ALL:
            for hop3 in ALL:
                if hop2 == 0 and hop3 == 0:
                    continue
                i = hop2 * 4 + hop3
                copies2[c, i].wait_recv()
                code = r2[c][i].astype(jnp.int32)
                total = total + decoded(code, power(code[14:15].astype(jnp.float32)))
        o_ref[:, pl.ds(col, cols)] = total[0:14]

    landed = 0

    def land(upto):
        nonlocal landed
        while landed < upto:
            swaps[landed].wait_recv()
            landed += 1

    screen_swap.wait_recv()
    peer_mask = mask_of(peer_screen)
    land(4)
    along_y = turns[0]
    prepare(along_y[0], 0, DEPTH, peer_mask)
    unit(2, 0)
    emit(2, 0)
    unit(0, 0)
    emit(0, 0)
    prepare(along_y[1], 1, DEPTH, peer_mask)
    prepare(along_y[2], 2, DEPTH, peer_mask)
    unit_by_place(1)
    unit_by_place(3)
    unit_by_place(2)
    emit(1, 0)
    unit(2, 1)
    emit(1, 1)
    unit(0, 1)
    emit(2, 1)
    set_exponents()
    unit(2, 2)
    emit(0, 1)
    emit(1, 2)
    prepare(along_y[3], 3, DEPTH, peer_mask)
    unit(0, 2)
    emit(2, 2)
    emit(1, 3)
    plane(2, 0)
    unit(2, 3)
    emit(0, 2)
    plane(0, 0)
    unit(0, 3)
    emit(2, 3)
    unit_by_place(0)
    emit(0, 3)
    plane(1, 0)
    plane(0, 1)
    plane(1, 1)
    plane(2, 1)
    plane(1, 2)
    plane(0, 2)
    plane(2, 2)
    plane(1, 3)
    plane(0, 3)
    plane(2, 3)
    for copy in sent[:-45]:
        copy.wait_send()
    last(0)
    last(1)
    last(2)
    for copy in sent[-45:]:
        copy.wait_send()


def on_device(factors, screen):
    f32, i16, bf16 = jnp.float32, jnp.int16, jnp.bfloat16
    v = pltpu.VMEM
    dma = pltpu.SemaphoreType.DMA
    widths = [c[2] for c in COLOURS]

    def each(shape, dtype):
        return [v((*shape, w), dtype) for w in widths]

    scratch = [
        v((2 * DEPTH, NBF), bf16), v((4, 384, DEPTH), bf16), v((224, 224), bf16),
        v((4, 224, 2 * DEPTH), bf16), v((4, 224, 2 * DEPTH), bf16), *[v((4, 56, widths[0]), f32)] * 4,
        v((4, 4, 56, widths[1]), f32), *[v((4, 56, widths[2]), f32)] * 4,
        *each((3, 4, 56), i16), *each((3, 4, 56), i16),
        *each((16, 16), i16), *each((16, 16), i16), *each((4, 4, 16), f32),
        v((1, 18), jnp.int32), v((1, 18), jnp.int32), v((8, 128), f32), v((8, 128), f32), v((8, 128), f32),
        v((9, 8, 128), f32), v((3, 8, 128), f32),
        dma((5,)), dma((9,)), dma((9,)), dma((3, 3, 4)), dma((3, 3, 4)), dma((3, 16)), dma((3, 16)),
        dma((9,)), dma((9,)),
    ]
    return pl.pallas_call(
        kernel,
        out_shape=jax.ShapeDtypeStruct((14, NBF), f32),
        in_specs=[pl.BlockSpec(memory_space=pltpu.HBM)] * 2,
        out_specs=pl.BlockSpec(memory_space=pltpu.VMEM),
        scratch_shapes=scratch,
        compiler_params=pltpu.CompilerParams(
            collective_id=0, has_side_effects=True, vmem_limit_bytes=55000000
        ),
    )(factors.reshape(ROWS, NBF), screen)


def solution(mesh):
    placed = (P(("grp", "mem"), None, None), P(("grp", "mem"), None))
    return jax.shard_map(
        on_device, mesh=mesh, in_specs=placed, out_specs=P(("grp", "mem"), None), check_vma=False
    )
```
